128 devices in a mesh: chan: 4 (over x), az: 8 (over z, y_lo), rng: 4 (over y_hi, core).
Axes of the slice: x: 4, y: 4 (y_hi: 2, y_lo: 2; y = y_hi * 2 + y_lo), z: 4, core: 2. Of those that a mesh axis runs over, the one named last changes fastest.
Arguments:
- raw: float32 [2, 16, 256, 16384], P(None, 'chan', 'rng', 'az'), may hold values from -6 to 6
- taps: float32 [2, 17, 256], P(None, None, 'rng'), may hold values from -1.5 to 1.5
- recon: float32 [2, 16, 16, 16384], P(None, 'az', None, ('chan', 'rng')), may hold values from -1 to 1
- channel_slot: int32 [16], replicated, may hold values from 0 to 15, each once
Outputs:
- reconstructed: float32 [2, 16, 4, 64, 16384], P(None, None, None, 'az', ('chan', 'rng'))
The draws below stay inside these ranges and needn't reach their ends.
Inputs may be any that keep to these rules, and one draw needn't show every extreme that they name: `channel_slot`: a permutation of the channels.
All inputs are finite; a program needn't handle non-finite values.
Results may differ from the reference program's by a relative error of at most 0.0003.
Values sent between devices are 32-bit elements; how exact they have to be, the bound alone decides.
A program may use at most 192 MiB of HBM per device.

```python
import jax
import jax.numpy as jnp
from jax import lax

CH = 16
NA = 16384
TAPS = 17
RSTRIP = 64
NR = 256
N_RNG = 4


def block_scale(stream_key, dims, split, least, high):
    def one(axis_at, shards_of):
        heights = jax.random.uniform(jax.random.fold_in(jax.random.fold_in(stream_key, 6), axis_at), (shards_of,), jnp.float32, least / len(split), high / len(split))
        return jnp.repeat(jnp.exp(heights), dims[axis_at] // shards_of).reshape((-1,) + (1,) * (len(dims) - axis_at - 1))

    loudness = one(*split[0])
    for cut in split[1:]:
        loudness = loudness * one(*cut)
    return loudness


def centred(rng, shape, scale, most, cuts=(), kind=jnp.bfloat16):
    values = jax.random.normal(rng, shape, jnp.float32) * scale
    if len(cuts) > 0:
        values = block_scale(rng, shape, cuts, -0.22, 0.18) * values
    return jnp.clip(values, min=-most, max=most).astype(kind)


def setup_inputs(seed: int = 0) -> dict:
    key_list = jax.random.split(jax.random.key(seed), 5)
    raw = centred(key_list[0], (2, CH, NR, NA), 1.0, 6.0, ((1, 4), (2, 4), (3, 8)), jnp.float32)
    taps = centred(key_list[1], (2, TAPS, NR), 0.25, 1.5, ((2, 4),), jnp.float32)
    recon = centred(key_list[2], (2, CH, CH, NA), (2 * CH) ** -0.5, 1.0, ((1, 8), (3, 16)), jnp.float32)
    channel_slot = jax.random.permutation(key_list[3], CH).astype(jnp.int32)
    return dict(raw=raw, taps=taps, recon=recon, channel_slot=channel_slot)


def reference(raw, taps, recon, channel_slot):
    width = taps.shape[1]
    half = (width - 1) // 2
    padded = jnp.pad(raw, ((0, 0), (0, 0), (half, half), (0, 0)))
    arranged = jnp.take(recon, channel_slot, axis=2)

    def strip(index):
        start = (index * RSTRIP).astype(jnp.int32)
        block = lax.dynamic_slice_in_dim(padded, start, RSTRIP + 2 * half, 2)
        coeffs = lax.dynamic_slice_in_dim(taps, start, RSTRIP, 2)
        real_part = jnp.zeros((CH, RSTRIP, NA), raw.dtype)
        imag_part = jnp.zeros((CH, RSTRIP, NA), raw.dtype)
        for offset in range(width):
            seg_real = block[0, :, offset:offset + RSTRIP, :]
            seg_imag = block[1, :, offset:offset + RSTRIP, :]
            tap_real = coeffs[0, offset][None, :, None]
            tap_imag = coeffs[1, offset][None, :, None]
            real_part = real_part + tap_real * seg_real - tap_imag * seg_imag
            imag_part = imag_part + tap_real * seg_imag + tap_imag * seg_real
        spectrum = jnp.fft.fft(real_part + 1j * imag_part, axis=-1, norm="ortho")
        spec_real = jnp.real(spectrum)
        spec_imag = jnp.imag(spectrum)
        high = lax.Precision.HIGHEST
        out_real = jnp.einsum("kcf,crf->krf", arranged[0], spec_real, precision=high) - jnp.einsum("kcf,crf->krf", arranged[1], spec_imag, precision=high)
        out_imag = jnp.einsum("kcf,crf->krf", arranged[0], spec_imag, precision=high) + jnp.einsum("kcf,crf->krf", arranged[1], spec_real, precision=high)
        return jnp.stack([out_real, out_imag])

    blocks = lax.map(strip, jnp.arange(N_RNG, dtype=jnp.int32))
    return jnp.moveaxis(blocks, 0, 2)
```

```python
import functools
import math

import jax
import jax.numpy as jnp
import ml_dtypes
import numpy as np
from jax import lax
from jax.experimental import pallas as pl
from jax.experimental.pallas import tpu as pltpu
from jax.sharding import PartitionSpec as P

MESH = pl.DeviceIdType.MESH
LANES = 128
BF = jnp.bfloat16
F32 = jnp.float32


def tables():
    n = np.arange(LANES)
    angle = 2.0 * np.pi * (np.outer(n, n) % LANES) / LANES
    cos, sin = np.cos(angle), np.sin(angle)
    dft = np.block([[cos, sin], [-sin, cos]])
    turn = 2.0 * np.pi * np.outer(n, n) / (LANES * LANES)
    scale = 1.0 / LANES
    twist = np.stack([np.cos(turn), np.sin(turn)]) * scale
    high = dft.astype(ml_dtypes.bfloat16)
    low = (dft - high.astype(np.float64)).astype(ml_dtypes.bfloat16)
    return np.stack([high, low]), twist.astype(np.float32)


def split(x):
    high = x.astype(BF)
    low = (x - high.astype(F32)).astype(BF)
    return high, low


def product(a, b, dims):
    dot = functools.partial(
        lax.dot_general, dimension_numbers=(dims, ((), ())), preferred_element_type=F32
    )
    return dot(a[0], b[0]) + (dot(a[1], b[0]) + dot(a[0], b[1]))


def kernel(
    raw, taps, recon, slot, dft, twist,
    out,
    xbuf, sbuf, rbuf, ubuf, dbuf, mbuf, acc, band, dftv, twv, tapv,
    load_sem, const_sem, m_ls, halo_ss, halo_rs, a_ss, a_rs, a_ls, m_ss, m_rs,
    c_ss, c_rs, c_ls, out_sem,
):
    ca, aa, ra = lax.axis_index("chan"), lax.axis_index("az"), lax.axis_index("rng")
    n_chan, n_az, n_rng = (lax.axis_size(a) for a in ("chan", "az", "rng"))
    chunks, half = raw.shape[1], (taps.shape[1] - 1) // 2
    rows, width = raw.shape[2], raw.shape[3]
    padded = rows + 2 * half
    group = rows // n_az
    tiles = width // LANES
    az_peers = [lax.rem(aa + d, n_az) for d in range(1, n_az)]
    c_peers = [
        (lax.rem(ca + dc, n_chan), lax.rem(ra + dr, n_rng))
        for dc in range(n_chan) for dr in range(n_rng) if dc or dr
    ]

    loads = [
        pltpu.make_async_copy(raw.at[:, m], xbuf.at[m, :, pl.ds(half, rows)], load_sem.at[m])
        for m in range(chunks)
    ]
    consts = [
        pltpu.make_async_copy(taps, tapv, const_sem.at[0]),
        pltpu.make_async_copy(dft, dftv, const_sem.at[1]),
        pltpu.make_async_copy(twist, twv, const_sem.at[2]),
    ]
    mats = [
        pltpu.make_async_copy(
            recon.at[:, :, :, pl.ds(f * LANES, LANES)], mbuf.at[aa, :, :, f], m_ls.at[f]
        )
        for f in range(group)
    ]
    for cp in [consts[0], loads[0]] + mats + loads[1:] + consts[1:]:
        cp.start()

    barrier = pltpu.get_barrier_semaphore()
    for a in az_peers:
        pl.semaphore_signal(barrier, inc=1, device_id=(ca, a, ra), device_id_type=MESH)
    for c, r in c_peers:
        pl.semaphore_signal(barrier, inc=1, device_id=(c, aa, r), device_id_type=MESH)

    @pl.when(ra == 0)
    def _():
        for m in range(chunks):
            xbuf[m, :, 0:half, :] = jnp.zeros((2, half, width), F32)

    @pl.when(ra == n_rng - 1)
    def _():
        for m in range(chunks):
            xbuf[m, :, padded - half :, :] = jnp.zeros((2, half, width), F32)

    pl.semaphore_wait(barrier, len(az_peers) + len(c_peers))

    def halo(m, side):
        src = raw.at[:, m, pl.ds(rows - half if side == 0 else 0, half)]
        dst = xbuf.at[m, :, pl.ds(0 if side == 0 else padded - half, half)]
        to = lax.rem(ra + (1 if side == 0 else n_rng - 1), n_rng)
        return pltpu.make_async_remote_copy(
            src, dst, halo_ss.at[m, side], halo_rs.at[m, side],
            device_id=(ca, aa, to), device_id_type=MESH,
        )

    for m in range(chunks):
        @pl.when(ra < n_rng - 1)
        def _():
            halo(m, 0).start()

        @pl.when(ra > 0)
        def _():
            halo(m, 1).start()

    pair = aa + 1 - 2 * lax.rem(aa, 2)
    for cp in mats:
        cp.wait()
    to_pair = pltpu.make_async_remote_copy(
        mbuf.at[aa], mbuf.at[aa], m_ss.at[0], m_rs.at[0], device_id=(ca, pair, ra), device_id_type=MESH
    )
    to_pair.start()

    consts[0].wait()
    top = jnp.concatenate([tapv[0], tapv[1]], axis=-1)
    bottom = jnp.concatenate([-tapv[1], tapv[0]], axis=-1)
    lane = lax.broadcasted_iota(jnp.int32, (padded, 2 * rows), 1)
    off = lax.broadcasted_iota(jnp.int32, (padded, 2 * rows), 0) - lax.rem(lane, rows)
    first = jnp.zeros((padded, 2 * rows), F32)
    second = jnp.zeros((padded, 2 * rows), F32)
    for j in range(2 * half + 1):
        hit = off == j
        first = jnp.where(hit, top[j : j + 1, :], first)
        second = jnp.where(hit, bottom[j : j + 1, :], second)
    rest = jnp.zeros((2 * LANES - 2 * padded, 2 * rows), F32)
    matrix = jnp.concatenate([first, second, rest], axis=0).T[:, : 2 * padded]
    high, low = split(matrix)
    band[0] = high
    band[1] = low
    acc[...] = jnp.zeros(acc.shape, F32)

    def a_copy(m, d):
        a = az_peers[d]
        return pltpu.make_async_remote_copy(
            sbuf.at[m, a], rbuf.at[m, :, pl.ds(aa * tiles, tiles)], a_ss.at[m, d], a_rs.at[m, d],
            device_id=(ca, a, ra), device_id_type=MESH,
        )

    def a_local(m):
        return pltpu.make_async_copy(
            sbuf.at[m, aa], rbuf.at[m, :, pl.ds(aa * tiles, tiles)], a_ls.at[m]
        )

    def filtered(m):
        def body(t, carry):
            lanes = pl.ds(pl.multiple_of(t * 2 * LANES, 2 * LANES), 2 * LANES)
            x = jnp.concatenate([xbuf[m, 0, :, lanes], xbuf[m, 1, :, lanes]], axis=0)
            y = product((band[0], band[1]), split(x), ((1,), (0,)))
            for p in range(2):
                for a in range(n_az):
                    at = p * rows + a * group
                    for i in range(2):
                        sbuf[m, a, p, t * 2 + i] = y[at : at + group, i * LANES : (i + 1) * LANES]
            return carry

        lax.fori_loop(0, tiles // 2, body, 0)

    for m in range(chunks):
        loads[m].wait()

        @pl.when(ra > 0)
        def _():
            halo(m, 0).wait_recv()

        @pl.when(ra < n_rng - 1)
        def _():
            halo(m, 1).wait_recv()

        filtered(m)
        for d in range(n_az - 1):
            a_copy(m, d).start()
        a_local(m).start()

    to_pair.wait_recv()

    def m_copy(d, which):
        to = lax.rem(aa + 2 * d, n_az)
        block = aa if which == 0 else pair
        i = 1 + 2 * (d - 1) + which
        return pltpu.make_async_remote_copy(
            mbuf.at[block], mbuf.at[block], m_ss.at[i], m_rs.at[i],
            device_id=(ca, to, ra), device_id_type=MESH,
        )

    passed = [m_copy(d, w) for d in range(1, n_az // 2) for w in range(2)]
    for cp in passed:
        cp.start()

    consts[1].wait()
    consts[2].wait()

    def c_copy(m, i):
        c, r = c_peers[i]
        return pltpu.make_async_remote_copy(
            ubuf.at[m, c * n_rng + r], dbuf.at[m, ca, ra], c_ss.at[m, i], c_rs.at[m, i],
            device_id=(c, aa, r), device_id_type=MESH,
        )

    def c_local(m):
        return pltpu.make_async_copy(ubuf.at[m, ca * n_rng + ra], dbuf.at[m, ca, ra], c_ls.at[m])

    def spectrum(m):
        src = rbuf.reshape(chunks, 2, LANES * group, LANES)
        dst = ubuf.reshape(chunks, n_chan * n_rng, 2, group * group, LANES)

        def body(b, carry):
            q = b * 2
            parts = [
                [src[m, p, pl.ds(q + i, LANES, stride=group), :] for i in range(2)]
                for p in range(2)
            ]
            x = jnp.concatenate([jnp.concatenate(part, axis=1) for part in parts], axis=0)
            y = product((dftv[0], dftv[1]), split(x), ((1,), (0,)))
            turned = []
            for i in range(2):
                re = y[:LANES, i * LANES : (i + 1) * LANES]
                im = y[LANES:, i * LANES : (i + 1) * LANES]
                turned.append(jnp.concatenate(
                    [re * twv[0] + im * twv[1], im * twv[0] - re * twv[1]], axis=1
                ))
            z = product((dftv[0], dftv[1]), split(jnp.concatenate(turned, axis=0)), ((1,), (1,)))
            for p in range(2):
                for to in range(n_chan * n_rng):
                    at = p * LANES + to * group
                    for i in range(2):
                        dst[m, to, p, pl.ds(q + i, group, stride=group), :] = (
                            z[at : at + group, i * LANES : (i + 1) * LANES]
                        )
            return carry

        lax.fori_loop(0, group // 2, body, 0)

    for m in range(chunks):
        a_local(m).wait()
        for d in range(n_az - 1):
            a_copy(m, d).wait_recv()
        spectrum(m)
        for i in range(len(c_peers)):
            c_copy(m, i).start()
        c_local(m).start()

    for cp in passed:
        cp.wait_recv()

    kb = 4

    def reconstruct(m, b):
        k0 = b * kb
        slots = [slot[c * chunks + m] for c in range(n_chan)]

        def body(f, carry):
            lanes = pl.ds(pl.multiple_of(f * LANES, LANES), LANES)
            total = [[[acc[p, k0 + k, s, :, lanes] for s in range(n_rng)] for k in range(kb)]
                     for p in range(2)]
            for c in range(n_chan):
                data = [[dbuf[m, c, s, p, f] for s in range(n_rng)] for p in range(2)]
                for k in range(kb):
                    az, kk = (k0 + k) // 2, k % 2
                    re = mbuf[az, 0, kk, f, pl.ds(slots[c], group, stride=0), :]
                    im = mbuf[az, 1, kk, f, pl.ds(slots[c], group, stride=0), :]
                    for s in range(n_rng):
                        total[0][k][s] = total[0][k][s] + re * data[0][s] - im * data[1][s]
                        total[1][k][s] = total[1][k][s] + re * data[1][s] + im * data[0][s]
            for p in range(2):
                for k in range(kb):
                    for s in range(n_rng):
                        acc[p, k0 + k, s, :, lanes] = total[p][k][s]
            return carry

        lax.fori_loop(0, group, body, 0)

    blocks = acc.shape[1] // kb

    def out_copy(b):
        part = pl.ds(b * kb, kb)
        return pltpu.make_async_copy(acc.at[:, part], out.at[:, part], out_sem.at[b])

    for m in range(chunks):
        c_local(m).wait()
        for i in range(len(c_peers)):
            c_copy(m, i).wait_recv()
        for b in range(blocks):
            reconstruct(m, b)
            if m == chunks - 1:
                out_copy(b).start()

    for m in range(chunks):
        @pl.when(ra < n_rng - 1)
        def _():
            halo(m, 0).wait_send()

        @pl.when(ra > 0)
        def _():
            halo(m, 1).wait_send()

        for d in range(n_az - 1):
            a_copy(m, d).wait_send()
        for i in range(len(c_peers)):
            c_copy(m, i).wait_send()
    to_pair.wait_send()
    for cp in passed:
        cp.wait_send()
    for b in range(blocks):
        out_copy(b).wait()


def shards(raw, taps, recon, channel_slot):
    n_chan, n_az, n_rng = (lax.axis_size(a) for a in ("chan", "az", "rng"))
    chunks, rows, width = raw.shape[1:]
    half = (taps.shape[1] - 1) // 2
    padded = rows + 2 * half
    group, tiles = rows // n_az, width // LANES
    subs, bins = recon.shape[1] * n_az, recon.shape[3]
    dft, twist = tables()
    sem = pltpu.SemaphoreType.DMA
    peers = n_chan * n_rng - 1
    return pl.pallas_call(
        kernel,
        out_shape=jax.ShapeDtypeStruct((2, subs, n_rng, group, bins), F32),
        in_specs=[
            pl.BlockSpec(memory_space=pl.ANY),
            pl.BlockSpec(memory_space=pl.ANY),
            pl.BlockSpec(memory_space=pl.ANY),
            pl.BlockSpec(memory_space=pltpu.SMEM),
            pl.BlockSpec(memory_space=pl.ANY),
            pl.BlockSpec(memory_space=pl.ANY),
        ],
        out_specs=pl.BlockSpec(memory_space=pl.ANY),
        scratch_shapes=[
            pltpu.VMEM((chunks, 2, padded, width), F32),
            pltpu.VMEM((chunks, n_az, 2, tiles, group, LANES), F32),
            pltpu.VMEM((chunks, 2, n_az * tiles, group, LANES), F32),
            pltpu.VMEM((chunks, n_chan * n_rng, 2, group, group, LANES), F32),
            pltpu.VMEM((chunks, n_chan, n_rng, 2, group, group, LANES), F32),
            pltpu.VMEM((n_az, 2, recon.shape[1], bins // LANES, recon.shape[2], LANES), F32),
            pltpu.VMEM((2, subs, n_rng, group, bins), F32),
            pltpu.VMEM((2, 2 * rows, 2 * padded), BF),
            pltpu.VMEM(dft.shape, BF),
            pltpu.VMEM(twist.shape, F32),
            pltpu.VMEM(taps.shape, F32),
            sem((chunks,)),
            sem((3,)),
            sem((bins // LANES,)),
            sem((chunks, 2)),
            sem((chunks, 2)),
            sem((chunks, n_az - 1)),
            sem((chunks, n_az - 1)),
            sem((chunks,)),
            sem((n_az - 1,)),
            sem((n_az - 1,)),
            sem((chunks, peers)),
            sem((chunks, peers)),
            sem((chunks,)),
            sem((subs // 4,)),
        ],
        compiler_params=pltpu.CompilerParams(
            collective_id=0, has_side_effects=True, vmem_limit_bytes=56 * 2**20
        ),
    )(raw, taps, recon, channel_slot, jnp.asarray(dft), jnp.asarray(twist))


def solution(mesh):
    return jax.shard_map(
        shards,
        mesh=mesh,
        in_specs=(
            P(None, "chan", "rng", "az"),
            P(None, None, "rng"),
            P(None, "az", None, ("chan", "rng")),
            P(),
        ),
        out_specs=P(None, None, None, "az", ("chan", "rng")),
        check_vma=False,
    )
```

```python
import functools
import math

import jax
import jax.numpy as jnp
import ml_dtypes
import numpy as np
from jax import lax
from jax.experimental import pallas as pl
from jax.experimental.pallas import tpu as pltpu
from jax.sharding import PartitionSpec as P

MESH = pl.DeviceIdType.MESH
LANES = 128
KB = 4
EARLY = 2
BF = jnp.bfloat16
F32 = jnp.float32


def tables():
    n = np.arange(LANES)
    angle = 2.0 * np.pi * (np.outer(n, n) % LANES) / LANES
    cos, sin = np.cos(angle), np.sin(angle)
    dft = np.block([[cos, sin], [-sin, cos]])
    turn = 2.0 * np.pi * np.outer(n, n) / (LANES * LANES)
    scale = 1.0 / LANES
    twist = np.stack([np.cos(turn), np.sin(turn)]) * scale
    high = dft.astype(ml_dtypes.bfloat16)
    low = (dft - high.astype(np.float64)).astype(ml_dtypes.bfloat16)
    return np.stack([high, low]), twist.astype(np.float32)


def split(x):
    high = x.astype(BF)
    low = (x - high.astype(F32)).astype(BF)
    return high, low


def product(a, b, dims):
    dot = functools.partial(
        lax.dot_general, dimension_numbers=(dims, ((), ())), preferred_element_type=F32
    )
    return dot(a[0], b[0]) + (dot(a[1], b[0]) + dot(a[0], b[1]))


def reconstruct(src, dst, data_ref, mats, sources, slots, first, count):
    n_rng, _, group = data_ref.shape[1:4]

    def body(at, carry):
        f, b = lax.rem(at, group), at // group
        lanes = pl.ds(pl.multiple_of(f * LANES, LANES), LANES)
        k0 = (first + b) * KB
        for k in range(KB):
            total = [[src[p, k0 + k, s, :, lanes] for s in range(n_rng)] for p in range(2)]
            for c, j in zip(sources, slots):
                az, kk = (k0 + k) // 2, k % 2
                re = mats[az, 0, kk, f, pl.ds(j, group, stride=0), :]
                im = mats[az, 1, kk, f, pl.ds(j, group, stride=0), :]
                for s in range(n_rng):
                    x, y = data_ref[c, s, 0, f], data_ref[c, s, 1, f]
                    total[0][s] = total[0][s] + re * x - im * y
                    total[1][s] = total[1][s] + re * y + im * x
            for p in range(2):
                for s in range(n_rng):
                    dst[p, k0 + k, s, :, lanes] = total[p][s]
        return carry

    lax.fori_loop(0, group * count, body, 0)


def finish(acc, dlast, mats, slot, out, res, sems):
    n_chan, subs = dlast.shape[0], acc.shape[1]
    chunks = slot.shape[0] // n_chan
    ca = lax.axis_index("chan")
    late = [lax.rem(ca + n_chan - d, n_chan) for d in range(EARLY, n_chan)]
    slots = [slot[c * chunks + chunks - 1] for c in late]
    block = subs // sems.shape[0]
    copies = []
    for b in range(sems.shape[0]):
        reconstruct(acc, res, dlast, mats, late, slots, b * block // KB, block // KB)
        part = pl.ds(b * block, block)
        copies.append(pltpu.make_async_copy(res.at[:, part], out.at[:, part], sems.at[b]))
        copies[b].start()
    for cp in copies:
        cp.wait()


def kernel(
    raw, taps, recon, slot, dft, twist,
    acc, dlast, mbuf,
    xbuf, sbuf, tbuf, rbuf, ubuf, dbuf, band, dftv, twv, tapv,
    load_sem, const_sem, m_ls, halo_ss, halo_rs, a_ss, a_rs, a_ls, t_ss, t_rs, m_ss, m_rs,
    c_ss, c_rs, c_ls, ready,
):
    ca, aa, ra = lax.axis_index("chan"), lax.axis_index("az"), lax.axis_index("rng")
    n_chan, n_az, n_rng = (lax.axis_size(a) for a in ("chan", "az", "rng"))
    chunks, half = raw.shape[1], (taps.shape[0] - 1) // 2
    rows, width = raw.shape[2], raw.shape[3]
    padded = rows + 2 * half
    group = rows // n_az
    tiles = width // LANES
    az_peers = [lax.rem(aa + d, n_az) for d in range(1, n_az)]
    core, side_y = lax.rem(ra, 2), ra // 2
    across = (1 - side_y) * 2
    chans = [lax.rem(ca + d, n_chan) for d in range(n_chan)]
    c_peers = [(c, lax.rem(ra + dr, n_rng)) for c in chans for dr in range(n_rng)][1:]
    pair = aa + 1 - 2 * lax.rem(aa, 2)
    near = [(ca, pair, ra)]
    near += [(ca, a, ra) for a in az_peers[1::2]]
    near += [(ca, aa, across + k) for k in range(2)]
    near += [(c, aa, side_y * 2 + k) for c in chans[1:] for k in range(2)]
    near += [(ca, aa, side_y * 2 + 1 - core)]

    loads = [
        pltpu.make_async_copy(raw.at[:, m], xbuf.at[m, :, pl.ds(half, rows)], load_sem.at[m])
        for m in range(chunks)
    ]
    consts = [
        pltpu.make_async_copy(taps, tapv, const_sem.at[0]),
        pltpu.make_async_copy(dft, dftv, const_sem.at[1]),
        pltpu.make_async_copy(twist, twv, const_sem.at[2]),
    ]
    mats = [
        pltpu.make_async_copy(
            recon.at[:, :, :, pl.ds(f * LANES, LANES)], mbuf.at[aa, :, :, f], m_ls.at[f]
        )
        for f in range(group)
    ]
    for cp in [consts[0], loads[0]] + mats + loads[1:] + consts[1:]:
        cp.start()

    barrier = pltpu.get_barrier_semaphore()
    for device in near:
        pl.semaphore_signal(barrier, inc=1, device_id=device, device_id_type=MESH)

    @pl.when(ra == 0)
    def _():
        for m in range(chunks):
            xbuf[m, :, 0:half, :] = jnp.zeros((2, half, width), F32)

    @pl.when(ra == n_rng - 1)
    def _():
        for m in range(chunks):
            xbuf[m, :, padded - half :, :] = jnp.zeros((2, half, width), F32)

    pl.semaphore_wait(barrier, len(near))

    def halo(m, side):
        src = xbuf.at[m, :, pl.ds(rows if side == 0 else half, half)]
        dst = xbuf.at[m, :, pl.ds(0 if side == 0 else padded - half, half)]
        to = lax.rem(ra + (1 if side == 0 else n_rng - 1), n_rng)
        return pltpu.make_async_remote_copy(
            src, dst, halo_ss.at[m, side], halo_rs.at[m, side],
            device_id=(ca, aa, to), device_id_type=MESH,
        )

    for m in range(chunks):
        loads[m].wait()

        @pl.when(ra < n_rng - 1)
        def _():
            halo(m, 0).start()

        @pl.when(ra > 0)
        def _():
            halo(m, 1).start()

    for cp in mats:
        cp.wait()
    to_pair = pltpu.make_async_remote_copy(
        mbuf.at[aa], mbuf.at[aa], m_ss.at[0], m_rs.at[0], device_id=(ca, pair, ra), device_id_type=MESH
    )
    to_pair.start()

    for c in chans[1:]:
        pl.semaphore_signal(ready, inc=1, device_id=(c, aa, ra), device_id_type=MESH)

    consts[0].wait()
    top = jnp.concatenate([tapv[:, 0], tapv[:, 1]], axis=-1)
    bottom = jnp.concatenate([-tapv[:, 1], tapv[:, 0]], axis=-1)
    lane = lax.broadcasted_iota(jnp.int32, (padded, 2 * rows), 1)
    off = lax.broadcasted_iota(jnp.int32, (padded, 2 * rows), 0) - lax.rem(lane, rows)
    first = jnp.zeros((padded, 2 * rows), F32)
    second = jnp.zeros((padded, 2 * rows), F32)
    for j in range(2 * half + 1):
        hit = off == j
        first = jnp.where(hit, top[j : j + 1, :], first)
        second = jnp.where(hit, bottom[j : j + 1, :], second)
    rest = jnp.zeros((2 * LANES - 2 * padded, 2 * rows), F32)
    matrix = jnp.concatenate([first, second, rest], axis=0).T[:, : 2 * padded]
    high, low = split(matrix)
    band[0] = high
    band[1] = low
    acc[...] = jnp.zeros(acc.shape, F32)

    n_z = n_az // 2
    far = [2, 1, 3]

    def remote(src, dst, send, recv, to):
        return pltpu.make_async_remote_copy(
            src, dst, send, recv, device_id=(ca, to, ra), device_id_type=MESH
        )

    def along_z(block, d):
        return lax.rem(block + 2 * d, n_az)

    def spot(m, source):
        return rbuf.at[m, :, pl.ds(source * tiles, tiles)]

    def z_copy(m, d):
        to = along_z(aa, d)
        return remote(sbuf.at[m, to], spot(m, aa), a_ss.at[m, d], a_rs.at[m, d], to)

    def y_copy(m):
        return remote(sbuf.at[m, pair], spot(m, aa), a_ss.at[m, 0], a_rs.at[m, 0], pair)

    def stage(m, d):
        src = sbuf.at[m, along_z(pair, d)]
        return remote(src, tbuf.at[m, d - 1], t_ss.at[m, d - 1], t_rs.at[m, d - 1], pair)

    def forward(m, d):
        i = n_z + d - 1
        return remote(tbuf.at[m, d - 1], spot(m, pair), a_ss.at[m, i], a_rs.at[m, i], along_z(aa, d))

    def a_copies(m):
        return [y_copy(m)] + [f(m, d) for f in (z_copy, forward) for d in far]

    def a_local(m):
        return pltpu.make_async_copy(
            sbuf.at[m, aa], rbuf.at[m, :, pl.ds(aa * tiles, tiles)], a_ls.at[m]
        )

    def filtered(m):
        def body(t, carry):
            lanes = pl.ds(pl.multiple_of(t * 2 * LANES, 2 * LANES), 2 * LANES)
            x = jnp.concatenate([xbuf[m, 0, :, lanes], xbuf[m, 1, :, lanes]], axis=0)
            y = product((band[0], band[1]), split(x), ((1,), (0,)))
            for p in range(2):
                for a in range(n_az):
                    at = p * rows + a * group
                    for i in range(2):
                        sbuf[m, a, p, t * 2 + i] = y[at : at + group, i * LANES : (i + 1) * LANES]
            return carry

        lax.fori_loop(0, tiles // 2, body, 0)

    for m in range(chunks):
        @pl.when(ra > 0)
        def _():
            halo(m, 0).wait_recv()

        @pl.when(ra < n_rng - 1)
        def _():
            halo(m, 1).wait_recv()

        filtered(m)
        for d in far:
            stage(m, d).start()
            z_copy(m, d).start()
        y_copy(m).start()
        a_local(m).start()

    to_pair.wait_recv()

    def m_copy(d, which):
        to = lax.rem(aa + 2 * d, n_az)
        block = aa if which == 0 else pair
        i = 1 + 2 * (d - 1) + which
        return pltpu.make_async_remote_copy(
            mbuf.at[block], mbuf.at[block], m_ss.at[i], m_rs.at[i],
            device_id=(ca, to, ra), device_id_type=MESH,
        )

    passed = [m_copy(d, w) for d in range(1, n_az // 2) for w in range(2)]
    for cp in passed:
        cp.start()

    consts[1].wait()
    consts[2].wait()
    pl.semaphore_wait(ready, n_chan - 1)

    def landing(m):
        return dlast.at[ca, ra] if m == chunks - 1 else dbuf.at[m, ca, ra]

    def c_copy(m, i):
        c, r = c_peers[i]
        return pltpu.make_async_remote_copy(
            ubuf.at[m, c * n_rng + r], landing(m), c_ss.at[m, i], c_rs.at[m, i],
            device_id=(c, aa, r), device_id_type=MESH,
        )

    def c_local(m):
        return pltpu.make_async_copy(ubuf.at[m, ca * n_rng + ra], landing(m), c_ls.at[m])

    def spectrum(m):
        src = rbuf.reshape(chunks, 2, LANES * group, LANES)
        dst = ubuf.reshape(chunks, n_chan * n_rng, 2, group * group, LANES)

        def body(b, carry):
            q = b * 2
            parts = [
                [src[m, p, pl.ds(q + i, LANES, stride=group), :] for i in range(2)]
                for p in range(2)
            ]
            x = jnp.concatenate([jnp.concatenate(part, axis=1) for part in parts], axis=0)
            y = product((dftv[0], dftv[1]), split(x), ((1,), (0,)))
            turned = []
            for i in range(2):
                re = y[:LANES, i * LANES : (i + 1) * LANES]
                im = y[LANES:, i * LANES : (i + 1) * LANES]
                turned.append(jnp.concatenate(
                    [re * twv[0] + im * twv[1], im * twv[0] - re * twv[1]], axis=1
                ))
            z = product((dftv[0], dftv[1]), split(jnp.concatenate(turned, axis=0)), ((1,), (1,)))
            for p in range(2):
                for to in range(n_chan * n_rng):
                    at = p * LANES + to * group
                    for i in range(2):
                        dst[m, to, p, pl.ds(q + i, group, stride=group), :] = (
                            z[at : at + group, i * LANES : (i + 1) * LANES]
                        )
            return carry

        lax.fori_loop(0, group // 2, body, 0)

    for m in range(chunks):
        a_local(m).wait()
        for d in far:
            stage(m, d).wait_recv()
            forward(m, d).start()
        for cp in a_copies(m):
            cp.wait_recv()
        spectrum(m)
        for i in range(len(c_peers)):
            c_copy(m, i).start()
        c_local(m).start()

    for cp in passed:
        cp.wait_recv()

    def c_wait(m, d):
        if d == 0:
            c_local(m).wait()
        for dr in range(n_rng):
            if d or dr:
                c_copy(m, d * n_rng + dr - 1).wait_recv()

    def add(m, ds):
        for d in ds:
            c_wait(m, d)
        sources = [lax.rem(ca + n_chan - d, n_chan) for d in ds]
        slots = [slot[c * chunks + m] for c in sources]
        data = dlast if m == chunks - 1 else dbuf.at[m]
        reconstruct(acc, acc, data, mbuf, sources, slots, 0, acc.shape[1] // KB)

    for m in range(chunks - 1):
        add(m, range(n_chan))
    if EARLY:
        add(chunks - 1, range(EARLY))
    for d in range(EARLY, n_chan):
        c_wait(chunks - 1, d)

    for m in range(chunks):
        @pl.when(ra < n_rng - 1)
        def _():
            halo(m, 0).wait_send()

        @pl.when(ra > 0)
        def _():
            halo(m, 1).wait_send()

        for cp in a_copies(m) + [stage(m, d) for d in far]:
            cp.wait_send()
        for i in range(len(c_peers)):
            c_copy(m, i).wait_send()
    to_pair.wait_send()
    for cp in passed:
        cp.wait_send()


def shards(raw, taps, recon, channel_slot):
    taps = jnp.transpose(taps, (1, 0, 2))
    n_chan, n_az, n_rng = (lax.axis_size(a) for a in ("chan", "az", "rng"))
    chunks, rows, width = raw.shape[1:]
    half = (taps.shape[0] - 1) // 2
    padded = rows + 2 * half
    group, tiles = rows // n_az, width // LANES
    subs, bins = recon.shape[1] * n_az, recon.shape[3]
    dft, twist = tables()
    sem = pltpu.SemaphoreType.DMA
    peers = n_chan * n_rng - 1
    vmem = pl.BlockSpec(memory_space=pltpu.VMEM)
    acc, dlast, mats = pl.pallas_call(
        kernel,
        out_shape=(
            pltpu.VMEM((2, subs, n_rng, group, bins), F32),
            pltpu.VMEM((n_chan, n_rng, 2, group, group, LANES), F32),
            pltpu.VMEM((n_az, 2, recon.shape[1], bins // LANES, recon.shape[2], LANES), F32),
        ),
        in_specs=[
            pl.BlockSpec(memory_space=pl.ANY),
            pl.BlockSpec(memory_space=pl.ANY),
            pl.BlockSpec(memory_space=pl.ANY),
            pl.BlockSpec(memory_space=pltpu.SMEM),
            pl.BlockSpec(memory_space=pl.ANY),
            pl.BlockSpec(memory_space=pl.ANY),
        ],
        out_specs=(vmem, vmem, vmem),
        scratch_shapes=[
            pltpu.VMEM((chunks, 2, padded, width), F32),
            pltpu.VMEM((chunks, n_az, 2, tiles, group, LANES), F32),
            pltpu.VMEM((chunks, n_az // 2 - 1, 2, tiles, group, LANES), F32),
            pltpu.VMEM((chunks, 2, n_az * tiles, group, LANES), F32),
            pltpu.VMEM((chunks, n_chan * n_rng, 2, group, group, LANES), F32),
            pltpu.VMEM((chunks - 1, n_chan, n_rng, 2, group, group, LANES), F32),
            pltpu.VMEM((2, 2 * rows, 2 * padded), BF),
            pltpu.VMEM(dft.shape, BF),
            pltpu.VMEM(twist.shape, F32),
            pltpu.VMEM(taps.shape, F32),
            sem((chunks,)),
            sem((3,)),
            sem((bins // LANES,)),
            sem((chunks, 2)),
            sem((chunks, 2)),
            sem((chunks, n_az - 1)),
            sem((chunks, n_az - 1)),
            sem((chunks,)),
            sem((chunks, n_az // 2 - 1)),
            sem((chunks, n_az // 2 - 1)),
            sem((n_az - 1,)),
            sem((n_az - 1,)),
            sem((chunks, peers)),
            sem((chunks, peers)),
            sem((chunks,)),
            pltpu.SemaphoreType.REGULAR,
        ],
        compiler_params=pltpu.CompilerParams(
            collective_id=0, has_side_effects=True, vmem_limit_bytes=52 * 2**20
        ),
    )(raw, taps, recon, channel_slot, jnp.asarray(dft), jnp.asarray(twist))
    return pl.pallas_call(
        finish,
        out_shape=jax.ShapeDtypeStruct((2, subs, n_rng, group, bins), F32),
        in_specs=[vmem, vmem, vmem, pl.BlockSpec(memory_space=pltpu.SMEM)],
        out_specs=pl.BlockSpec(memory_space=pl.ANY),
        scratch_shapes=[pltpu.VMEM((2, subs, n_rng, group, bins), F32), sem((subs // 4,))],
        compiler_params=pltpu.CompilerParams(vmem_limit_bytes=16 * 2**20),
    )(acc, dlast, mats, channel_slot)


def solution(mesh):
    return jax.shard_map(
        shards,
        mesh=mesh,
        in_specs=(
            P(None, "chan", "rng", "az"),
            P(None, None, "rng"),
            P(None, "az", None, ("chan", "rng")),
            P(),
        ),
        out_specs=P(None, None, None, "az", ("chan", "rng")),
        check_vma=False,
    )
```

```python
import functools
import math

import jax
import jax.numpy as jnp
import ml_dtypes
import numpy as np
from jax import lax
from jax.experimental import pallas as pl
from jax.experimental.pallas import tpu as pltpu
from jax.sharding import PartitionSpec as P

MESH = pl.DeviceIdType.MESH
LANES = 128
KB = 4
EARLY = 2
ORDER = (0, 2, 1, 3)
BF = jnp.bfloat16
F32 = jnp.float32


def tables():
    n = np.arange(LANES)
    angle = 2.0 * np.pi * (np.outer(n, n) % LANES) / LANES
    cos, sin = np.cos(angle), np.sin(angle)
    dft = np.block([[cos, sin], [-sin, cos]])
    turn = 2.0 * np.pi * np.outer(n, n) / (LANES * LANES)
    scale = 1.0 / LANES
    twist = np.stack([np.cos(turn), np.sin(turn)]) * scale
    high = dft.astype(ml_dtypes.bfloat16)
    low = (dft - high.astype(np.float64)).astype(ml_dtypes.bfloat16)
    return np.stack([high, low]), twist.astype(np.float32)


def split(x):
    high = x.astype(BF)
    low = (x - high.astype(F32)).astype(BF)
    return high, low


def product(a, b, dims):
    dot = functools.partial(
        lax.dot_general, dimension_numbers=(dims, ((), ())), preferred_element_type=F32
    )
    return dot(a[0], b[0]) + (dot(a[1], b[0]) + dot(a[0], b[1]))


def reconstruct(src, dst, data_ref, mats, sources, slots, first, count):
    n_rng, _, group = data_ref.shape[1:4]

    def body(at, carry):
        f, b = lax.rem(at, group), at // group
        lanes = pl.ds(pl.multiple_of(f * LANES, LANES), LANES)
        k0 = (first + b) * KB
        for k in range(KB):
            total = [[src[p, k0 + k, s, :, lanes] for s in range(n_rng)] for p in range(2)]
            for c, j in zip(sources, slots):
                az, kk = (k0 + k) // 2, k % 2
                re = mats[az, 0, kk, f, pl.ds(j, group, stride=0), :]
                im = mats[az, 1, kk, f, pl.ds(j, group, stride=0), :]
                for s in range(n_rng):
                    x, y = data_ref[c, s, 0, f], data_ref[c, s, 1, f]
                    total[0][s] = total[0][s] + re * x - im * y
                    total[1][s] = total[1][s] + re * y + im * x
            for p in range(2):
                for s in range(n_rng):
                    dst[p, k0 + k, s, :, lanes] = total[p][s]
        return carry

    lax.fori_loop(0, group * count, body, 0)


def finish(acc, dlast, mats, slot, out, res, sems):
    n_chan, subs = dlast.shape[0], acc.shape[1]
    chunks = slot.shape[0] // n_chan
    ca = lax.axis_index("chan")
    late = [lax.rem(ca + n_chan - d, n_chan) for d in ORDER[EARLY:]]
    slots = [slot[c * chunks + chunks - 1] for c in late]
    block = subs // sems.shape[0]
    copies = []
    for b in range(sems.shape[0]):
        reconstruct(acc, res, dlast, mats, late, slots, b * block // KB, block // KB)
        part = pl.ds(b * block, block)
        copies.append(pltpu.make_async_copy(res.at[:, part], out.at[:, part], sems.at[b]))
        copies[b].start()
    for cp in copies:
        cp.wait()


def kernel(
    raw, taps, recon, slot, dft, twist,
    acc, dlast, mbuf,
    xbuf, sbuf, tbuf, rbuf, ubuf, dbuf, band, dftv, twv, tapv,
    load_sem, const_sem, m_ls, halo_ss, halo_rs, a_ss, a_rs, a_ls, t_ss, t_rs, m_ss, m_rs,
    c_ss, c_rs, c_ls, ready,
):
    ca, aa, ra = lax.axis_index("chan"), lax.axis_index("az"), lax.axis_index("rng")
    n_chan, n_az, n_rng = (lax.axis_size(a) for a in ("chan", "az", "rng"))
    chunks, half = raw.shape[1], (taps.shape[0] - 1) // 2
    rows, width = raw.shape[2], raw.shape[3]
    padded = rows + 2 * half
    group = rows // n_az
    tiles = width // LANES
    az_peers = [lax.rem(aa + d, n_az) for d in range(1, n_az)]
    core, side_y = lax.rem(ra, 2), ra // 2
    across = (1 - side_y) * 2
    chans = [lax.rem(ca + d, n_chan) for d in range(n_chan)]
    c_peers = [(c, lax.rem(ra + dr, n_rng)) for c in [chans[d] for d in ORDER] for dr in range(n_rng)][1:]
    pair = aa + 1 - 2 * lax.rem(aa, 2)
    near = [(ca, pair, ra)]
    near += [(ca, a, ra) for a in az_peers[1::2]]
    near += [(ca, aa, across + k) for k in range(2)]
    near += [(c, aa, side_y * 2 + k) for c in chans[1:] for k in range(2)]
    near += [(ca, aa, side_y * 2 + 1 - core)]

    loads = [
        pltpu.make_async_copy(raw.at[:, m], xbuf.at[m, :, pl.ds(half, rows)], load_sem.at[m])
        for m in range(chunks)
    ]
    consts = [
        pltpu.make_async_copy(taps, tapv, const_sem.at[0]),
        pltpu.make_async_copy(dft, dftv, const_sem.at[1]),
        pltpu.make_async_copy(twist, twv, const_sem.at[2]),
    ]
    mats = [
        pltpu.make_async_copy(
            recon.at[:, :, :, pl.ds(f * LANES, LANES)], mbuf.at[aa, :, :, f], m_ls.at[f]
        )
        for f in range(group)
    ]
    for cp in [consts[0], loads[0]] + mats + loads[1:] + consts[1:]:
        cp.start()

    barrier = pltpu.get_barrier_semaphore()
    for device in near:
        pl.semaphore_signal(barrier, inc=1, device_id=device, device_id_type=MESH)

    @pl.when(ra == 0)
    def _():
        for m in range(chunks):
            xbuf[m, :, 0:half, :] = jnp.zeros((2, half, width), F32)

    @pl.when(ra == n_rng - 1)
    def _():
        for m in range(chunks):
            xbuf[m, :, padded - half :, :] = jnp.zeros((2, half, width), F32)

    pl.semaphore_wait(barrier, len(near))

    def halo(m, side):
        src = xbuf.at[m, :, pl.ds(rows if side == 0 else half, half)]
        dst = xbuf.at[m, :, pl.ds(0 if side == 0 else padded - half, half)]
        to = lax.rem(ra + (1 if side == 0 else n_rng - 1), n_rng)
        return pltpu.make_async_remote_copy(
            src, dst, halo_ss.at[m, side], halo_rs.at[m, side],
            device_id=(ca, aa, to), device_id_type=MESH,
        )

    for m in range(chunks):
        loads[m].wait()

        @pl.when(ra < n_rng - 1)
        def _():
            halo(m, 0).start()

        @pl.when(ra > 0)
        def _():
            halo(m, 1).start()

    for cp in mats:
        cp.wait()
    to_pair = pltpu.make_async_remote_copy(
        mbuf.at[aa], mbuf.at[aa], m_ss.at[0], m_rs.at[0], device_id=(ca, pair, ra), device_id_type=MESH
    )
    to_pair.start()

    for c in chans[1:]:
        pl.semaphore_signal(ready, inc=1, device_id=(c, aa, ra), device_id_type=MESH)

    consts[0].wait()
    top = jnp.concatenate([tapv[:, 0], tapv[:, 1]], axis=-1)
    bottom = jnp.concatenate([-tapv[:, 1], tapv[:, 0]], axis=-1)
    lane = lax.broadcasted_iota(jnp.int32, (padded, 2 * rows), 1)
    off = lax.broadcasted_iota(jnp.int32, (padded, 2 * rows), 0) - lax.rem(lane, rows)
    first = jnp.zeros((padded, 2 * rows), F32)
    second = jnp.zeros((padded, 2 * rows), F32)
    for j in range(2 * half + 1):
        hit = off == j
        first = jnp.where(hit, top[j : j + 1, :], first)
        second = jnp.where(hit, bottom[j : j + 1, :], second)
    rest = jnp.zeros((2 * LANES - 2 * padded, 2 * rows), F32)
    matrix = jnp.concatenate([first, second, rest], axis=0).T[:, : 2 * padded]
    high, low = split(matrix)
    band[0] = high
    band[1] = low
    acc[...] = jnp.zeros(acc.shape, F32)

    n_z = n_az // 2
    far = [2, 1, 3]

    def remote(src, dst, send, recv, to):
        return pltpu.make_async_remote_copy(
            src, dst, send, recv, device_id=(ca, to, ra), device_id_type=MESH
        )

    def along_z(block, d):
        return lax.rem(block + 2 * d, n_az)

    def spot(m, source):
        return rbuf.at[m, :, pl.ds(source * tiles, tiles)]

    def z_copy(m, d):
        to = along_z(aa, d)
        return remote(sbuf.at[m, to], spot(m, aa), a_ss.at[m, d], a_rs.at[m, d], to)

    def y_copy(m):
        return remote(sbuf.at[m, pair], spot(m, aa), a_ss.at[m, 0], a_rs.at[m, 0], pair)

    def stage(m, d):
        src = sbuf.at[m, along_z(pair, d)]
        return remote(src, tbuf.at[m, d - 1], t_ss.at[m, d - 1], t_rs.at[m, d - 1], pair)

    def forward(m, d):
        i = n_z + d - 1
        return remote(tbuf.at[m, d - 1], spot(m, pair), a_ss.at[m, i], a_rs.at[m, i], along_z(aa, d))

    def a_copies(m):
        return [y_copy(m)] + [f(m, d) for f in (z_copy, forward) for d in far]

    def a_local(m):
        return pltpu.make_async_copy(
            sbuf.at[m, aa], rbuf.at[m, :, pl.ds(aa * tiles, tiles)], a_ls.at[m]
        )

    def filtered(m):
        def body(t, carry):
            lanes = pl.ds(pl.multiple_of(t * 2 * LANES, 2 * LANES), 2 * LANES)
            x = jnp.concatenate([xbuf[m, 0, :, lanes], xbuf[m, 1, :, lanes]], axis=0)
            y = product((band[0], band[1]), split(x), ((1,), (0,)))
            for p in range(2):
                for a in range(n_az):
                    at = p * rows + a * group
                    for i in range(2):
                        sbuf[m, a, p, t * 2 + i] = y[at : at + group, i * LANES : (i + 1) * LANES]
            return carry

        lax.fori_loop(0, tiles // 2, body, 0)

    for m in range(chunks):
        @pl.when(ra > 0)
        def _():
            halo(m, 0).wait_recv()

        @pl.when(ra < n_rng - 1)
        def _():
            halo(m, 1).wait_recv()

        filtered(m)
        for d in far:
            stage(m, d).start()
            z_copy(m, d).start()
        y_copy(m).start()
        a_local(m).start()

    to_pair.wait_recv()

    def m_copy(d, which):
        to = lax.rem(aa + 2 * d, n_az)
        block = aa if which == 0 else pair
        i = 1 + 2 * (d - 1) + which
        return pltpu.make_async_remote_copy(
            mbuf.at[block], mbuf.at[block], m_ss.at[i], m_rs.at[i],
            device_id=(ca, to, ra), device_id_type=MESH,
        )

    passed = [m_copy(d, w) for d in range(1, n_az // 2) for w in range(2)]
    for cp in passed:
        cp.start()

    consts[1].wait()
    consts[2].wait()
    pl.semaphore_wait(ready, n_chan - 1)

    def landing(m):
        return dlast.at[ca, ra] if m == chunks - 1 else dbuf.at[m, ca, ra]

    def c_copy(m, i):
        c, r = c_peers[i]
        return pltpu.make_async_remote_copy(
            ubuf.at[m, c * n_rng + r], landing(m), c_ss.at[m, i], c_rs.at[m, i],
            device_id=(c, aa, r), device_id_type=MESH,
        )

    def c_local(m):
        return pltpu.make_async_copy(ubuf.at[m, ca * n_rng + ra], landing(m), c_ls.at[m])

    def c_start(m):
        for i in range(len(c_peers)):
            c_copy(m, i).start()
        c_local(m).start()

    def spectrum(m):
        src = rbuf.reshape(chunks, 2, LANES * group, LANES)
        dst = ubuf.reshape(chunks, n_chan * n_rng, 2, group * group, LANES)

        def body(b, carry):
            q = b * 2
            parts = [
                [src[m, p, pl.ds(q + i, LANES, stride=group), :] for i in range(2)]
                for p in range(2)
            ]
            x = jnp.concatenate([jnp.concatenate(part, axis=1) for part in parts], axis=0)
            y = product((dftv[0], dftv[1]), split(x), ((1,), (0,)))
            turned = []
            for i in range(2):
                re = y[:LANES, i * LANES : (i + 1) * LANES]
                im = y[LANES:, i * LANES : (i + 1) * LANES]
                turned.append(jnp.concatenate(
                    [re * twv[0] + im * twv[1], im * twv[0] - re * twv[1]], axis=1
                ))
            z = product((dftv[0], dftv[1]), split(jnp.concatenate(turned, axis=0)), ((1,), (1,)))
            for p in range(2):
                for to in range(n_chan * n_rng):
                    at = p * LANES + to * group
                    for i in range(2):
                        dst[m, to, p, pl.ds(q + i, group, stride=group), :] = (
                            z[at : at + group, i * LANES : (i + 1) * LANES]
                        )
            return carry

        lax.fori_loop(0, group // 2, body, 0)

    for m in range(chunks):
        a_local(m).wait()
        for d in far:
            stage(m, d).wait_recv()
            forward(m, d).start()
        if m:
            c_start(m - 1)
        for cp in a_copies(m):
            cp.wait_recv()
        spectrum(m)
        if m == chunks - 1:
            c_start(m)

    for cp in passed:
        cp.wait_recv()

    def c_wait(m, d):
        if d == 0:
            c_local(m).wait()
        for dr in range(n_rng):
            if d or dr:
                c_copy(m, d * n_rng + dr - 1).wait_recv()

    def add(m, ds):
        for d in ds:
            c_wait(m, d)
        sources = [lax.rem(ca + n_chan - ORDER[d], n_chan) for d in ds]
        slots = [slot[c * chunks + m] for c in sources]
        data = dlast if m == chunks - 1 else dbuf.at[m]
        reconstruct(acc, acc, data, mbuf, sources, slots, 0, acc.shape[1] // KB)

    for m in range(chunks - 1):
        add(m, range(n_chan))
    if EARLY:
        add(chunks - 1, range(EARLY))
    for d in range(EARLY, n_chan):
        c_wait(chunks - 1, d)

    for m in range(chunks):
        @pl.when(ra < n_rng - 1)
        def _():
            halo(m, 0).wait_send()

        @pl.when(ra > 0)
        def _():
            halo(m, 1).wait_send()

        for cp in a_copies(m) + [stage(m, d) for d in far]:
            cp.wait_send()
        for i in range(len(c_peers)):
            c_copy(m, i).wait_send()
    to_pair.wait_send()
    for cp in passed:
        cp.wait_send()


def shards(raw, taps, recon, channel_slot):
    taps = jnp.transpose(taps, (1, 0, 2))
    n_chan, n_az, n_rng = (lax.axis_size(a) for a in ("chan", "az", "rng"))
    chunks, rows, width = raw.shape[1:]
    half = (taps.shape[0] - 1) // 2
    padded = rows + 2 * half
    group, tiles = rows // n_az, width // LANES
    subs, bins = recon.shape[1] * n_az, recon.shape[3]
    dft, twist = tables()
    sem = pltpu.SemaphoreType.DMA
    peers = n_chan * n_rng - 1
    vmem = pl.BlockSpec(memory_space=pltpu.VMEM)
    acc, dlast, mats = pl.pallas_call(
        kernel,
        out_shape=(
            pltpu.VMEM((2, subs, n_rng, group, bins), F32),
            pltpu.VMEM((n_chan, n_rng, 2, group, group, LANES), F32),
            pltpu.VMEM((n_az, 2, recon.shape[1], bins // LANES, recon.shape[2], LANES), F32),
        ),
        in_specs=[
            pl.BlockSpec(memory_space=pl.ANY),
            pl.BlockSpec(memory_space=pl.ANY),
            pl.BlockSpec(memory_space=pl.ANY),
            pl.BlockSpec(memory_space=pltpu.SMEM),
            pl.BlockSpec(memory_space=pl.ANY),
            pl.BlockSpec(memory_space=pl.ANY),
        ],
        out_specs=(vmem, vmem, vmem),
        scratch_shapes=[
            pltpu.VMEM((chunks, 2, padded, width), F32),
            pltpu.VMEM((chunks, n_az, 2, tiles, group, LANES), F32),
            pltpu.VMEM((chunks, n_az // 2 - 1, 2, tiles, group, LANES), F32),
            pltpu.VMEM((chunks, 2, n_az * tiles, group, LANES), F32),
            pltpu.VMEM((chunks, n_chan * n_rng, 2, group, group, LANES), F32),
            pltpu.VMEM((chunks - 1, n_chan, n_rng, 2, group, group, LANES), F32),
            pltpu.VMEM((2, 2 * rows, 2 * padded), BF),
            pltpu.VMEM(dft.shape, BF),
            pltpu.VMEM(twist.shape, F32),
            pltpu.VMEM(taps.shape, F32),
            sem((chunks,)),
            sem((3,)),
            sem((bins // LANES,)),
            sem((chunks, 2)),
            sem((chunks, 2)),
            sem((chunks, n_az - 1)),
            sem((chunks, n_az - 1)),
            sem((chunks,)),
            sem((chunks, n_az // 2 - 1)),
            sem((chunks, n_az // 2 - 1)),
            sem((n_az - 1,)),
            sem((n_az - 1,)),
            sem((chunks, peers)),
            sem((chunks, peers)),
            sem((chunks,)),
            pltpu.SemaphoreType.REGULAR,
        ],
        compiler_params=pltpu.CompilerParams(
            collective_id=0, has_side_effects=True, vmem_limit_bytes=52 * 2**20
        ),
    )(raw, taps, recon, channel_slot, jnp.asarray(dft), jnp.asarray(twist))
    return pl.pallas_call(
        finish,
        out_shape=jax.ShapeDtypeStruct((2, subs, n_rng, group, bins), F32),
        in_specs=[vmem, vmem, vmem, pl.BlockSpec(memory_space=pltpu.SMEM)],
        out_specs=pl.BlockSpec(memory_space=pl.ANY),
        scratch_shapes=[pltpu.VMEM((2, subs, n_rng, group, bins), F32), sem((subs // 4,))],
        compiler_params=pltpu.CompilerParams(vmem_limit_bytes=16 * 2**20),
    )(acc, dlast, mats, channel_slot)


def solution(mesh):
    return jax.shard_map(
        shards,
        mesh=mesh,
        in_specs=(
            P(None, "chan", "rng", "az"),
            P(None, None, "rng"),
            P(None, "az", None, ("chan", "rng")),
            P(),
        ),
        out_specs=P(None, None, None, "az", ("chan", "rng")),
        check_vma=False,
    )
```
